32 devices in a mesh: section: 2 (over y), expert: 16 (over z, x, core).
Axes of the slice: x: 2, y: 2, z: 4, core: 2. Of those that a mesh axis runs over, the one named last changes fastest.
Arguments:
- reference_act: bfloat16 [2, 1024, 2048], P('section', 'expert'), may hold values from -6 to 6
- codes: int32 [2, 1024, 2048], P('section', 'expert'), may hold values from -127 to 127
- scale_index: int32 [2, 1024], P('section', 'expert'), may hold values from 0 to 15
- scale_table: float32 [16], replicated, may hold values from 0.002 to 0.02
- norm_gain: float32 [2, 2048], P('section'), may hold values from 0.25 to 1.75
- routes_fwd: int32 [2, 1024, 8], P('section', 'expert'), may hold values from 0 to 15, all different within a row; in each aligned block of 64 rows (0 to 63, 64 to 127, ..., all dimensions but the last counted through in order) at most 48 rows name the same one
- probs_fwd: float32 [2, 1024, 8], P('section', 'expert'), may hold values from 0.03 to 0.4
- gate_weight: bfloat16 [2, 16, 2048, 768], P('section', 'expert'), may hold values from -0.125 to 0.125
- up_weight: bfloat16 [2, 16, 2048, 768], P('section', 'expert'), may hold values from -0.125 to 0.125
- down_weight: bfloat16 [2, 16, 768, 2048], P('section', 'expert'), may hold values from -0.21875 to 0.21875
- saved_input: bfloat16 [2, 1024, 2048], P('section', 'expert'), may hold values from -6 to 6
- routes_bwd: int32 [2, 1024, 8], P('section', 'expert'), may hold values from 0 to 15, all different within a row; in each aligned block of 64 rows (0 to 63, 64 to 127, ..., all dimensions but the last counted through in order) at most 48 rows name the same one
- probs_bwd: float32 [2, 1024, 8], P('section', 'expert'), may hold values from 0.03 to 0.4
- saved_preact: bfloat16 [2, 16, 768, 1536], P('section', 'expert'), may hold values from -8 to 8
- cotangent: bfloat16 [2, 1024, 2048], P('section', 'expert'), may hold values from -6 to 6
Outputs:
- mixed: bfloat16 [2, 1024, 2048], P('section', 'expert')
- grad_input: bfloat16 [2, 1024, 2048], P('section', 'expert')
The draws below stay inside these ranges and needn't reach their ends.
Inputs may be any that keep to these rules, and one draw needn't show every extreme that they name: `routes_fwd`: the 8 ids of a token differ; among the tokens of one device no expert is named more than 48 times, a bound that some block reaches. `routes_bwd`: the 8 ids of a token differ; among the tokens of one device no expert is named more than 48 times, a bound that some block reaches.
All inputs are finite; a program needn't handle non-finite values.
Results may differ from the reference program's by a relative error of at most 0.0051.
Values may be sent and summed in bfloat16 or wider, within the bound.
No kernel may reach another device: no remote copies, remote signals or barrier semaphores. Data moves between devices by JAX's collectives and lax.ppermute only.
A program may use at most 128 MiB of HBM per device.

```python
import math
import jax
import jax.numpy as jnp
import numpy as np
from jax import lax

D = 2048
FF = 768
TOP = 8
TOK_DEV = 64
LEVELS = 16
SECTIONS = 2
EXPERTS = 16
TOKENS = 1024
CAP = 48


def touch_ends(array, own_key, least, top_value):
    shape = array.shape
    index_at = [jax.random.randint(jax.random.fold_in(own_key, axis), (), 0, shape[axis]) for axis in range(len(shape))]
    array = array.at[tuple(index_at)].set(least)
    longest = shape.index(max(shape))
    index_at[longest] = (index_at[longest] + 1) % shape[longest]
    return array.at[tuple(index_at)].set(top_value)


def steps_of(own_key, shape, shards, least, largest):
    def one(axis_at, blocks):
        steps = jax.random.uniform(jax.random.fold_in(jax.random.fold_in(own_key, 6), axis_at), (blocks,), jnp.float32, least / len(shards), largest / len(shards))
        return jnp.repeat(jnp.exp(steps), shape[axis_at] // blocks).reshape((-1,) + (1,) * (len(shape) - axis_at - 1))

    level = one(*shards[0])
    for cut in shards[1:]:
        level = level * one(*cut)
    return level


def routed_block(key, own, number, rows, count, top, limit, skew):
    ranking = jax.random.permutation(key, count)
    crowded, common = shares(count, rows * top, limit, skew, True), shares(count, rows * top, limit, skew, False)
    places = jnp.arange(count)

    def named(sizes, offset_by):
        used = int((sizes > 0).sum())
        fixed = max(1, used // 4)
        passed = fixed + (places - fixed + offset_by * (used - fixed)) % max(1, count - fixed)
        return jnp.zeros((count,), jnp.int32).at[ranking[jnp.where(places < fixed, places, passed)]].set(jnp.asarray(sizes, jnp.int32))

    sizes = jnp.where(number % 4 == 0, named(crowded, number // 4), named(common, number - number // 4 - 1))
    mixed = jax.random.permutation(jax.random.fold_in(own, 3), count)
    donor, taker = mixed[0:count // 2 * 2:2], mixed[1:count // 2 * 2:2]
    margin = jnp.minimum(sizes[donor] - 1, limit - sizes[taker]) // 2
    margin = jnp.where((donor == ranking[0]) | (taker == ranking[0]) | (sizes[taker] == 0), 0, jnp.maximum(margin, 0))
    passed = jax.random.randint(jax.random.fold_in(own, 4), (count // 2,), 0, 1 << 20) % (margin + 1)
    sizes = sizes.at[donor].add(-passed).at[taker].add(passed)
    items = jnp.searchsorted(jnp.cumsum(sizes), jnp.arange(rows * top), side="right").astype(jnp.int32)
    grid = items.reshape(top, rows).T
    grid = grid[jax.random.permutation(jax.random.fold_in(own, 1), rows)]
    offset_by = jax.random.randint(jax.random.fold_in(own, 2), (rows, 1), 0, top)
    return jnp.take_along_axis(grid, (jnp.arange(top)[None, :] + offset_by) % top, axis=1)


def shares(number_of, total, reach, lean, full):
    weights = [(1 << 20) // math.isqrt(rank ** lean) + 1 for rank in range(1, number_of + 1)]
    largest = reach if full else min(reach, max(-(-total // number_of), total * weights[0] // sum(weights)))
    least = 1 if total - largest >= number_of - 1 else 0
    counts, spare = [largest] + [least] * (number_of - 1), total - largest - least * (number_of - 1)
    while spare > 0:
        movable = [i for i in range(1, number_of) if counts[i] < largest] or [i for i in range(1, number_of) if counts[i] < reach]
        mass, budget = sum([weights[i] for i in movable]), spare
        for i in movable:
            addition = min(reach - counts[i], max(1, budget * weights[i] // mass), spare)
            counts[i] = counts[i] + addition
            spare = spare - addition
    return np.array(counts)


def normal_values(key, shape, width, most, cuts=(), kind=jnp.bfloat16):
    values = width * jax.random.normal(key, shape, jnp.float32)
    if cuts:
        values = values * steps_of(key, shape, cuts, -0.22, 0.18)
    return jnp.clip(values, -most, most).astype(kind)


def setup_inputs(seed: int = 0) -> dict:
    key_of = jax.random.split(jax.random.key(seed), 16)
    reference_act = normal_values(key_of[0], (SECTIONS, TOKENS, D), 1.0, 6.0, ((0, 2), (1, 16)))
    codes = touch_ends(jax.random.randint(key_of[1], (SECTIONS, TOKENS, D), -127, 128), jax.random.fold_in(key_of[1], 1), -127, 127).astype(jnp.int32)
    scale_index = touch_ends(jax.random.randint(key_of[2], (SECTIONS, TOKENS), 0, LEVELS), jax.random.fold_in(key_of[2], 1), 0, LEVELS - 1).astype(jnp.int32)
    scale_table = jnp.clip(jnp.exp(jax.random.uniform(key_of[3], (LEVELS,), jnp.float32, math.log(0.002), math.log(0.02))), 0.002, 0.02)
    norm_gain = jnp.clip(1.0 + 0.15 * jax.random.normal(key_of[4], (SECTIONS, D), jnp.float32), 0.25, 1.75)
    routes_fwd_keys = jax.random.split(jax.random.fold_in(key_of[5], 1), SECTIONS * TOKENS // TOK_DEV)
    routes_fwd_turns = jax.random.permutation(jax.random.fold_in(key_of[5], 3), SECTIONS * TOKENS // TOK_DEV)
    routes_fwd = jax.vmap(lambda own, number: routed_block(jax.random.fold_in(key_of[5], 2), own, number, TOK_DEV, EXPERTS, TOP, CAP, 2))(routes_fwd_keys, routes_fwd_turns).reshape((SECTIONS, TOKENS, TOP))
    probs_fwd = jnp.clip(jnp.exp(math.log(0.4) - 2.5902672 * jax.random.uniform(key_of[6], (SECTIONS, TOKENS, TOP), jnp.float32) ** steps_of(key_of[6], (SECTIONS, TOKENS, TOP), ((0, 2), (1, 16)), -0.2, 0.2)), 0.03, 0.4)
    gate_weight = normal_values(key_of[7], (SECTIONS, EXPERTS, D, FF), D ** -0.5, 0.125, ((0, 2), (1, 16)))
    up_weight = normal_values(key_of[8], (SECTIONS, EXPERTS, D, FF), D ** -0.5, 0.125, ((0, 2), (1, 16)))
    down_weight = normal_values(key_of[9], (SECTIONS, EXPERTS, FF, D), FF ** -0.5, 0.21875, ((0, 2), (1, 16)))
    saved_input = normal_values(key_of[10], (SECTIONS, TOKENS, D), 1.0, 6.0, ((0, 2), (1, 16)))
    routes_bwd_keys = jax.random.split(jax.random.fold_in(key_of[11], 1), SECTIONS * TOKENS // TOK_DEV)
    routes_bwd_turns = jax.random.permutation(jax.random.fold_in(key_of[11], 3), SECTIONS * TOKENS // TOK_DEV)
    routes_bwd = jax.vmap(lambda own, number: routed_block(jax.random.fold_in(key_of[11], 2), own, number, TOK_DEV, EXPERTS, TOP, CAP, 2))(routes_bwd_keys, routes_bwd_turns).reshape((SECTIONS, TOKENS, TOP))
    probs_bwd = jnp.clip(jnp.exp(math.log(0.4) - 2.5902672 * jax.random.uniform(key_of[12], (SECTIONS, TOKENS, TOP), jnp.float32) ** steps_of(key_of[12], (SECTIONS, TOKENS, TOP), ((0, 2), (1, 16)), -0.2, 0.2)), 0.03, 0.4)
    saved_preact = normal_values(key_of[13], (SECTIONS, EXPERTS, EXPERTS * CAP, 2 * FF), 1.5, 8.0, ((0, 2), (1, 16)))
    cotangent = normal_values(key_of[14], (SECTIONS, TOKENS, D), 1.0, 6.0, ((0, 2), (1, 16)))
    return {"reference_act": reference_act, "codes": codes, "scale_index": scale_index, "scale_table": scale_table, "norm_gain": norm_gain, "routes_fwd": routes_fwd, "probs_fwd": probs_fwd, "gate_weight": gate_weight, "up_weight": up_weight, "down_weight": down_weight, "saved_input": saved_input, "routes_bwd": routes_bwd, "probs_bwd": probs_bwd, "saved_preact": saved_preact, "cotangent": cotangent}


EPSILON = 1e-06

def inverse_rms(values):
    return lax.rsqrt(lax.optimization_barrier(jnp.mean(values * values, axis=-1, keepdims=True)) + EPSILON)

def slot_targets(routes, experts, capacity):
    flat_ids = routes.reshape(-1).astype(jnp.int32)
    onehot = (flat_ids[:, None] == jnp.arange(experts, dtype=jnp.int32)[None, :]).astype(jnp.int32)
    earlier = jnp.cumsum(onehot, axis=0) - onehot
    slot_index = lax.optimization_barrier(jnp.sum(earlier * onehot, axis=1))
    return (flat_ids * capacity + slot_index).astype(jnp.int32)

def dispatch(rows, targets, experts, capacity):
    copies_each = targets.shape[0] // rows.shape[0]
    copies = jnp.repeat(rows, copies_each, axis=0)
    buffer = jnp.zeros((experts * capacity, rows.shape[1]), rows.dtype)
    return buffer.at[targets].set(copies)

def collect(buffer, targets, weights):
    picked = buffer[targets].astype(jnp.float32).reshape(weights.shape[0], weights.shape[1], buffer.shape[1])
    return lax.optimization_barrier(jnp.sum(picked * weights[:, :, None], axis=1))

def expert_forward(rows, gate_matrix, up_matrix, down_matrix):
    gate_act = jnp.dot(rows, gate_matrix, preferred_element_type=jnp.float32)
    up_act = jnp.dot(rows, up_matrix, preferred_element_type=jnp.float32)
    hidden = (gate_act * jax.nn.sigmoid(gate_act) * up_act).astype(jnp.bfloat16)
    return jnp.dot(hidden, down_matrix, preferred_element_type=jnp.float32).astype(jnp.bfloat16)

def expert_backward(grad_rows, stored, gate_matrix, up_matrix, down_matrix):
    hidden_units = gate_matrix.shape[1]
    gate_act = stored[:, :hidden_units].astype(jnp.float32)
    up_act = stored[:, hidden_units:].astype(jnp.float32)
    contract = (((1,), (1,)), ((), ()))
    grad_hidden = lax.dot_general(grad_rows, down_matrix, contract, preferred_element_type=jnp.float32)
    sigma = jax.nn.sigmoid(gate_act)
    silu_value = gate_act * sigma
    slope = sigma * (1.0 + gate_act * (1.0 - sigma))
    grad_gate = (grad_hidden * up_act * slope).astype(jnp.bfloat16)
    grad_up = (grad_hidden * silu_value).astype(jnp.bfloat16)
    result = lax.dot_general(grad_gate, gate_matrix, contract, preferred_element_type=jnp.float32)
    result = result + lax.dot_general(grad_up, up_matrix, contract, preferred_element_type=jnp.float32)
    return result.astype(jnp.bfloat16)

def through_experts(rows, routes, weights, expert_fn, expert_args):
    model_width = rows.shape[1]
    blocks = rows.reshape(EXPERTS, TOK_DEV, model_width)
    targets = jax.vmap(lambda block_routes: slot_targets(block_routes, EXPERTS, CAP))(routes.reshape(EXPERTS, TOK_DEV, TOP))
    sent = jax.vmap(lambda block_rows, block_targets: dispatch(block_rows, block_targets, EXPERTS, CAP))(blocks, targets)
    arrived = sent.reshape(EXPERTS, EXPERTS, CAP, model_width).transpose(1, 0, 2, 3).reshape(EXPERTS, EXPERTS * CAP, model_width)
    produced = lax.map(lambda member: expert_fn(*member), (arrived,) + expert_args)
    returned = produced.reshape(EXPERTS, EXPERTS, CAP, model_width).transpose(1, 0, 2, 3).reshape(EXPERTS, EXPERTS * CAP, model_width)
    combined = jax.vmap(collect)(returned, targets, weights.reshape(EXPERTS, TOK_DEV, TOP))
    return combined.reshape(EXPERTS * TOK_DEV, model_width)

def reference(reference_act, codes, scale_index, scale_table, norm_gain, routes_fwd, probs_fwd, gate_weight, up_weight, down_weight, saved_input, routes_bwd, probs_bwd, saved_preact, cotangent):
    row_scale = scale_table[scale_index]
    delta_rows = (codes.astype(jnp.float32) * row_scale[:, :, None]).astype(jnp.bfloat16)
    received = jnp.concatenate([jnp.zeros_like(delta_rows[:1]), delta_rows[:-1]], axis=0)
    grad_out = jnp.roll(cotangent, -1, axis=0)
    outputs = []
    gradients = []
    for section_index in range(SECTIONS):
        inputs_now = reference_act[section_index].astype(jnp.float32) + received[section_index].astype(jnp.float32)
        gain_row = norm_gain[section_index]
        normed = (inputs_now * inverse_rms(inputs_now) * gain_row).astype(jnp.bfloat16)
        forward_args = (gate_weight[section_index], up_weight[section_index], down_weight[section_index])
        mixed = inputs_now + through_experts(normed, routes_fwd[section_index], probs_fwd[section_index], expert_forward, forward_args)
        outputs.append(mixed.astype(jnp.bfloat16))
        backward_args = (saved_preact[section_index], gate_weight[section_index], up_weight[section_index], down_weight[section_index])
        grad_normed = through_experts(grad_out[section_index], routes_bwd[section_index], probs_bwd[section_index], expert_backward, backward_args)
        saved_now = saved_input[section_index].astype(jnp.float32)
        scale_now = inverse_rms(saved_now)
        weighted = grad_normed * gain_row
        projection = lax.optimization_barrier(jnp.mean(weighted * saved_now, axis=-1, keepdims=True))
        grad_now = grad_out[section_index].astype(jnp.float32) + scale_now * weighted - saved_now * scale_now * scale_now * scale_now * projection
        gradients.append(grad_now.astype(jnp.bfloat16))
    return (jnp.stack(outputs), jnp.stack(gradients))
```

```python
import jax
import jax.numpy as jnp
import numpy as np
from jax import lax
from jax.experimental import pallas as pl
from jax.experimental.pallas import tpu as pltpu
from jax.sharding import PartitionSpec as P

EPSILON = 1e-06


def from_behind(block, axis, distance):
    devices = range(lax.axis_size(axis))
    route = [(i - distance, i) for i in devices if i - distance in devices]
    return lax.ppermute(block, axis, route)


def shifted(x, axis, by):
    size = lax.axis_size(axis)
    return lax.ppermute(x, axis, [(i, (i + by) % size) for i in range(size)])


def inverse_rms(values):
    return lax.rsqrt(jnp.mean(values * values, axis=-1, keepdims=True) + EPSILON)


class Grid:
    def __init__(self, size):
        self.size = size
        self.inner = 2 if size % 2 == 0 else 1
        self.mid = 2 if (size // self.inner) % 2 == 0 else 1
        self.unit = self.inner * self.mid
        self.outer = size // self.unit

    def around(self, x, steps):
        moved = steps * self.unit
        return lax.ppermute(x, "expert", [(i, (i + moved) % self.size) for i in range(self.size)])

    def across(self, x):
        return lax.ppermute(x, "expert", [(i, i ^ self.inner) for i in range(self.size)])

    def beside(self, x):
        return lax.ppermute(x, "expert", [(i, i ^ 1) for i in range(self.size)])

    def groups(self):
        order = sorted(range(self.outer), key=lambda d: (min(d, self.outer - d), d))
        return [order[i : i + 2] for i in range(0, self.outer, 2)]

    def numbers(self, group):
        steps = np.array([0] + list(group) * 4, np.int32)
        flips = [0] + [f for f in (0, self.inner, 1, 1 ^ self.inner) for _ in group]
        me = lax.axis_index("expert")
        return ((me - self.unit * steps) % self.size) ^ np.array(flips, np.int32)

    def gather(self, x):
        near = {d: x if d == 0 else self.around(x, d) for d in sum(self.groups(), [])}
        pieces = []
        for group in self.groups():
            own = jnp.concatenate([near[d] for d in group], axis=0)
            other = self.across(own)
            pieces.append((own, other, self.beside(own), self.beside(other)))
        return pieces

    def scatter_sum(self, partials):
        f32, bf16 = jnp.float32, jnp.bfloat16
        total = 0.0
        for group, (own, other, own_beside, other_beside) in zip(self.groups(), partials):
            sent = (other.astype(f32) + self.beside(other_beside).astype(f32)).astype(bf16)
            near = own.astype(f32) + self.beside(own_beside).astype(f32)
            near = near + self.across(sent).astype(f32)
            block = own.shape[0] // len(group)
            for i, d in enumerate(group):
                part = near[i * block : (i + 1) * block]
                if d:
                    part = self.around(part.astype(bf16), -d).astype(f32)
                total = total + part
        return total


NT = (((1,), (1,)), ((), ()))
VMEM = pl.BlockSpec(memory_space=pltpu.VMEM)
SMEM = pl.BlockSpec(memory_space=pltpu.SMEM)
ANY = pl.BlockSpec(memory_space=pl.ANY)


def own_weight(table, me, first, experts):
    lane = lax.broadcasted_iota(jnp.int32, table.shape, 1)
    high = first * experts + me
    here = (lane == high) | (lane == high + experts)
    return jnp.sum(jnp.where(here, table, 0.0), axis=1, keepdims=True)


def put_rows(out, outs):
    start = 0
    for ref in outs:
        ref[...] = out[start : start + ref.shape[0]]
        start += ref.shape[0]


def forward_kernel(experts, ids, a, b, c, d, ta, tb, tc, td, wg, wu, wd, oa, ob, oc, od, vg, vu, vd, sems):
    f32, bf16 = jnp.float32, jnp.bfloat16
    loads = [
        pltpu.make_async_copy(src, dst, sems.at[i])
        for i, (src, dst) in enumerate(((wg, vg), (wu, vu), (wd, vd)))
    ]
    for load in loads:
        load.start()
    table = jnp.concatenate([t[...] for t in (ta, tb, tc, td)], axis=0).astype(f32)
    weight = own_weight(table, ids[0], 0, experts)
    rows = jnp.concatenate([r[...] for r in (a, b, c, d)], axis=0)
    loads[0].wait()
    gate = jnp.dot(rows, vg[...], preferred_element_type=f32)
    loads[1].wait()
    up = jnp.dot(rows, vu[...], preferred_element_type=f32)
    hidden = (gate * jax.nn.sigmoid(gate) * up).astype(bf16)
    loads[2].wait()
    out = jnp.dot(hidden, vd[...], preferred_element_type=f32)
    put_rows((out * weight).astype(bf16), (oa, ob, oc, od))


def backward_kernel(
    experts, tokens, ids, a, b, c, d, stored, wg, wu, wd, oa, ob, oc, od, vg, vu, vd, vs, sems
):
    f32, bf16 = jnp.float32, jnp.bfloat16
    blocks, capacity = vs.shape[0], vs.shape[1]
    hidden_units = vg.shape[1]
    width = oa.shape[1]
    saves = [
        pltpu.make_async_copy(stored.at[ids[1 + i]], vs.at[i], sems.at[3 + i]) for i in range(blocks)
    ]
    loads = [
        pltpu.make_async_copy(src, dst, sems.at[i])
        for i, (src, dst) in enumerate(((wd, vd), (wg, vg), (wu, vu)))
    ]
    for load in loads[:1] + saves + loads[1:]:
        load.start()
    table = jnp.concatenate([r[:, width:] for r in (a, b, c, d)], axis=0).astype(f32)
    weight = own_weight(table, ids[0], 2, experts)
    rows = jnp.concatenate([r[:, :width] for r in (a, b, c, d)], axis=0)
    loads[0].wait()
    grad_hidden = lax.dot_general(rows, vd[...], NT, preferred_element_type=f32)

    below = lax.broadcasted_iota(jnp.int32, (tokens, tokens), 0)
    below = (below > lax.broadcasted_iota(jnp.int32, (tokens, tokens), 1)).astype(bf16)
    column = lax.broadcasted_iota(jnp.int32, (tokens, capacity), 1).astype(f32)
    gates, ups = [], []
    for save in saves:
        save.wait()
    for i in range(blocks):
        named = weight[i * tokens : (i + 1) * tokens] > 0
        ones = jnp.broadcast_to(jnp.where(named, 1.0, 0.0), (tokens, 128)).astype(bf16)
        earlier = jnp.dot(below, ones, preferred_element_type=f32)[:, :1]
        slot = jnp.where(named, earlier, -1.0)
        pick = (column == slot).astype(f32).astype(bf16)
        placed = jnp.dot(pick, vs[i], preferred_element_type=f32)
        gates.append(placed[:, :hidden_units])
        ups.append(placed[:, hidden_units:])
    gate = jnp.concatenate(gates, axis=0)
    up = jnp.concatenate(ups, axis=0)
    sigma = jax.nn.sigmoid(gate)
    grad_gate = (grad_hidden * up * sigma * (1.0 + gate * (1.0 - sigma))).astype(bf16)
    grad_up = (grad_hidden * gate * sigma).astype(bf16)
    loads[1].wait()
    out = lax.dot_general(grad_gate, vg[...], NT, preferred_element_type=f32)
    loads[2].wait()
    out = out + lax.dot_general(grad_up, vu[...], NT, preferred_element_type=f32)
    put_rows((out * weight).astype(bf16), (oa, ob, oc, od))


def expert_forward(ids, rows, carried, weights, experts):
    width = rows[0].shape[1]
    hidden_units = weights[0].shape[1]
    side = carried[0].shape[1] - width
    total = sum(r.shape[0] for r in rows)
    tables = [
        pl.BlockSpec((c.shape[0], side), lambda i, at=width // side: (0, at)) for c in carried
    ]
    whole = [pl.BlockSpec(r.shape, lambda i: (0, 0)) for r in rows]
    return pl.pallas_call(
        lambda *refs: forward_kernel(experts, *refs),
        grid=(1,),
        out_shape=[jax.ShapeDtypeStruct(r.shape, jnp.bfloat16) for r in rows],
        in_specs=[SMEM] + whole + tables + [ANY] * 3,
        out_specs=whole,
        scratch_shapes=[pltpu.VMEM(w.shape, w.dtype) for w in weights]
        + [pltpu.SemaphoreType.DMA((3,))],
        compiler_params=pltpu.CompilerParams(vmem_limit_bytes=40 << 20),
        cost_estimate=pl.CostEstimate(
            flops=6 * total * width * hidden_units, bytes_accessed=10 << 20, transcendentals=0
        ),
        name="expert_forward",
    )(ids, *rows, *carried, *weights)


def expert_backward(ids, carried, stored, weights, experts, tokens, width):
    hidden_units = weights[0].shape[1]
    total = sum(r.shape[0] for r in carried)
    blocks = total // tokens
    outs = [jax.ShapeDtypeStruct((c.shape[0], width), jnp.bfloat16) for c in carried]
    return pl.pallas_call(
        lambda *refs: backward_kernel(experts, tokens, *refs),
        out_shape=outs,
        in_specs=[SMEM] + [VMEM] * 4 + [ANY] * 4,
        out_specs=[VMEM] * 4,
        scratch_shapes=[pltpu.VMEM(w.shape, w.dtype) for w in weights]
        + [
            pltpu.VMEM((blocks,) + stored.shape[1:], stored.dtype),
            pltpu.SemaphoreType.DMA((3 + blocks,)),
        ],
        compiler_params=pltpu.CompilerParams(vmem_limit_bytes=48 << 20),
        cost_estimate=pl.CostEstimate(
            flops=6 * total * width * hidden_units, bytes_accessed=12 << 20, transcendentals=0
        ),
        name="expert_backward",
    )(ids, *carried, stored, *weights)


def dense_weights(routes, probs, experts):
    ids = jnp.arange(experts, dtype=jnp.int32)
    hit = routes[:, :, None] == ids[None, None, :]
    return jnp.sum(jnp.where(hit, probs[:, :, None], 0.0), axis=1)


def in_two(values):
    high = values.astype(jnp.bfloat16)
    low = (values - high.astype(jnp.float32)).astype(jnp.bfloat16)
    return [high, low]


def on_device(
    reference_act,
    codes,
    scale_index,
    scale_table,
    norm_gain,
    routes_fwd,
    probs_fwd,
    gate_weight,
    up_weight,
    down_weight,
    saved_input,
    routes_bwd,
    probs_bwd,
    saved_preact,
    cotangent,
):
    f32, bf16 = jnp.float32, jnp.bfloat16
    experts = lax.axis_size("expert")
    grid = Grid(experts)
    tokens, model_width = reference_act.shape[1:]
    levels = scale_table.shape[0]
    weights = (gate_weight[0, 0], up_weight[0, 0], down_weight[0, 0])
    stored = saved_preact[0, 0].reshape(experts, -1, saved_preact.shape[3])

    grad_out = shifted(cotangent[0], "section", -1)
    picker = (scale_index[0][:, None] == jnp.arange(levels, dtype=jnp.int32)[None, :]).astype(f32)
    row_scale = jnp.sum(picker * scale_table[None, :], axis=1)
    delta_rows = (codes[0].astype(f32) * row_scale[:, None]).astype(bf16)
    received = from_behind(delta_rows, "section", 1)

    table = in_two(dense_weights(routes_fwd[0], probs_fwd[0], experts))
    table += in_two(dense_weights(routes_bwd[0], probs_bwd[0], experts))
    table = jnp.concatenate(table, axis=1)
    table = jnp.pad(table, ((0, 0), (0, -table.shape[1] % 128)))
    carried = grid.gather(jnp.concatenate([grad_out, table], axis=1))

    inputs_now = reference_act[0].astype(f32) + received.astype(f32)
    gain_row = norm_gain[0]
    normed = (inputs_now * inverse_rms(inputs_now) * gain_row).astype(bf16)
    rows = grid.gather(normed)

    numbers = [grid.numbers(group) for group in grid.groups()]
    slot_grads = [
        expert_backward(ids, piece, stored, weights, experts, tokens, model_width)
        for ids, piece in zip(numbers, carried)
    ]
    grad_normed = grid.scatter_sum(slot_grads)
    produced = [
        expert_forward(ids, piece, side, weights, experts)
        for ids, piece, side in zip(numbers, rows, carried)
    ]
    mixed = inputs_now + grid.scatter_sum(produced)

    saved_now = saved_input[0].astype(f32)
    scale_now = inverse_rms(saved_now)
    weighted = grad_normed * gain_row
    projection = jnp.mean(weighted * saved_now, axis=-1, keepdims=True)
    grad_now = (
        grad_out.astype(f32)
        + scale_now * weighted
        - saved_now * scale_now * scale_now * scale_now * projection
    )
    return (mixed.astype(bf16)[None], grad_now.astype(bf16)[None])


def solution(mesh):
    return jax.shard_map(
        on_device,
        mesh=mesh,
        in_specs=(
            P("section", "expert", None),
            P("section", "expert", None),
            P("section", "expert"),
            P(),
            P("section", None),
            P("section", "expert", None),
            P("section", "expert", None),
            P("section", "expert", None, None),
            P("section", "expert", None, None),
            P("section", "expert", None, None),
            P("section", "expert", None),
            P("section", "expert", None),
            P("section", "expert", None),
            P("section", "expert", None, None),
            P("section", "expert", None),
        ),
        out_specs=(P("section", "expert", None), P("section", "expert", None)),
        check_vma=False,
    )
```

```python
import jax
import jax.numpy as jnp
import numpy as np
from jax import lax
from jax.experimental import pallas as pl
from jax.experimental.pallas import tpu as pltpu
from jax.sharding import PartitionSpec as P

EPSILON = 1e-06
NORM_FLOPS = 4_000_000_000
PREPARE_FLOPS = 8_000_000_000


def from_behind(block, axis, distance):
    devices = range(lax.axis_size(axis))
    route = [(i - distance, i) for i in devices if i - distance in devices]
    return lax.ppermute(block, axis, route)


def shifted(x, axis, by):
    size = lax.axis_size(axis)
    return lax.ppermute(x, axis, [(i, (i + by) % size) for i in range(size)])


def inverse_rms(values):
    return lax.rsqrt(jnp.mean(values * values, axis=-1, keepdims=True) + EPSILON)


class Grid:
    def __init__(self, size):
        assert size >= 8 and size & (size - 1) == 0
        self.size = size
        self.outer = size // 4
        self.groups = [(k, k + 1) for k in range(0, self.outer, 2)]

    def swap(self, x, bits):
        return lax.ppermute(x, "expert", [(i, i ^ bits) for i in range(self.size)])

    def numbers(self, group):
        flips = [0] + [4 * k + f for f in (0, 2, 1, 3) for k in group]
        return lax.axis_index("expert") ^ np.array(flips, np.int32)

    def gather(self, x):
        near = {0: x}
        for k in range(1, self.outer):
            low = k & -k
            near[k] = self.swap(near[k - low], 4 * low)
        pieces = []
        for group in self.groups:
            own = [near[k] for k in group]
            other, own_beside, other_beside = [], [], []
            for k in group:
                other.append(self.swap(near[k], 2))
                own_beside.append(self.swap(near[k], 1))
                other_beside.append(self.swap(other[-1], 1))
            pieces.append(own + other + own_beside + other_beside)
        return pieces

    def scatter_sum(self, partials):
        f32, bf16 = jnp.float32, jnp.bfloat16
        total = {}
        for group, piece in zip(self.groups, partials):
            own, other, own_beside, other_beside = piece
            other_beside = self.swap(other_beside, 1)
            own_beside = self.swap(own_beside, 1)
            sent = (other.astype(f32) + other_beside.astype(f32)).astype(bf16)
            crossed = self.swap(sent, 2)
            near = own.astype(f32) + own_beside.astype(f32) + crossed.astype(f32)
            block = own.shape[0] // len(group)
            for i, k in enumerate(group):
                total[k] = near[i * block : (i + 1) * block]
        for k in sorted(total, key=lambda k: (-bin(k).count("1"), -k)):
            low = k & -k
            if k:
                part = self.swap(total[k].astype(bf16), 4 * low)
                total[k - low] = total[k - low] + part.astype(f32)
        return total[0]


NT = (((1,), (1,)), ((), ()))
VMEM = pl.BlockSpec(memory_space=pltpu.VMEM)
SMEM = pl.BlockSpec(memory_space=pltpu.SMEM)
ANY = pl.BlockSpec(memory_space=pl.ANY)


def own_weight(table, me, first, experts):
    lane = lax.broadcasted_iota(jnp.int32, table.shape, 1)
    high = first * experts + me
    here = (lane == high) | (lane == high + experts)
    return jnp.sum(jnp.where(here, table, 0.0), axis=1, keepdims=True)


def put_rows(out, outs):
    start = 0
    for ref in outs:
        ref[...] = out[start : start + ref.shape[0]]
        start += ref.shape[0]


def forward_kernel(experts, pieces, ids, *refs):
    f32, bf16 = jnp.float32, jnp.bfloat16
    blocks, tables, refs = refs[:pieces], refs[pieces : 2 * pieces], refs[2 * pieces :]
    wg, wu, wd, oa, ob, oc, od = refs
    table = jnp.concatenate([t[...] for t in tables], axis=0).astype(f32)
    weight = own_weight(table, ids[0], 0, experts)
    rows = jnp.concatenate([r[...] for r in blocks], axis=0)
    gate = jnp.dot(rows, wg[...], preferred_element_type=f32)
    up = jnp.dot(rows, wu[...], preferred_element_type=f32)
    hidden = (gate * jax.nn.sigmoid(gate) * up).astype(bf16)
    out = jnp.dot(hidden, wd[...], preferred_element_type=f32)
    put_rows((out * weight).astype(bf16), (oa, ob, oc, od))


def prepare_kernel(ids, stored, slopes):
    hidden_units = stored.shape[2] // 2

    def block(i, carry):
        kept = stored[i].astype(jnp.float32)
        gate, up = kept[:, :hidden_units], kept[:, hidden_units:]
        sigma = jax.nn.sigmoid(gate)
        slope = up * sigma * (1.0 + gate * (1.0 - sigma))
        slopes[i] = jnp.concatenate([slope, gate * sigma], axis=1).astype(jnp.bfloat16)
        return carry

    lax.fori_loop(0, stored.shape[0], block, 0)


def prepare(ids, stored):
    return pl.pallas_call(
        prepare_kernel,
        out_shape=jax.ShapeDtypeStruct(stored.shape, stored.dtype),
        in_specs=[SMEM, VMEM],
        out_specs=VMEM,
        compiler_params=pltpu.CompilerParams(vmem_limit_bytes=12 << 20),
        cost_estimate=pl.CostEstimate(
            flops=PREPARE_FLOPS, bytes_accessed=4 * stored.size, transcendentals=stored.size
        ),
        name="prepare",
    )(ids, stored)


def backward_kernel(experts, pieces, ids, *refs):
    f32, bf16 = jnp.float32, jnp.bfloat16
    carried, refs = refs[:pieces], refs[pieces:]
    stored, wg, wu, wd, oa, ob, oc, od = refs
    capacity = stored.shape[1]
    tokens = carried[0].shape[0]
    hidden_units = wg.shape[1]
    width = oa.shape[1]
    table = jnp.concatenate([r[:, width:] for r in carried], axis=0).astype(f32)
    weight = own_weight(table, ids[0], 2, experts)
    rows = jnp.concatenate([r[:, :width] for r in carried], axis=0)

    below = lax.broadcasted_iota(jnp.int32, (tokens, tokens), 0)
    below = (below > lax.broadcasted_iota(jnp.int32, (tokens, tokens), 1)).astype(bf16)
    column = lax.broadcasted_iota(jnp.int32, (tokens, capacity), 1).astype(f32)
    grad_hidden = lax.dot_general(rows, wd[...], NT, preferred_element_type=f32)
    grad_gates, grad_ups = [], []
    for i in range(pieces):
        part = slice(i * tokens, (i + 1) * tokens)
        named = weight[part] > 0
        ones = jnp.broadcast_to(jnp.where(named, 1.0, 0.0), (tokens, 128)).astype(bf16)
        earlier = jnp.dot(below, ones, preferred_element_type=f32)[:, :1]
        slot = jnp.where(named, earlier, -1.0)
        pick = (column == slot).astype(f32).astype(bf16)
        placed = jnp.dot(pick, stored[ids[1 + i]], preferred_element_type=f32)
        hidden = grad_hidden[part]
        grad_gates.append((hidden * placed[:, :hidden_units]).astype(bf16))
        grad_ups.append((hidden * placed[:, hidden_units:]).astype(bf16))
    grad_gate = jnp.concatenate(grad_gates, axis=0)
    grad_up = jnp.concatenate(grad_ups, axis=0)
    out = lax.dot_general(grad_gate, wg[...], NT, preferred_element_type=f32)
    out = out + lax.dot_general(grad_up, wu[...], NT, preferred_element_type=f32)
    put_rows((out * weight).astype(bf16), (oa, ob, oc, od))


def expert_forward(ids, rows, carried, weights, experts):
    width = rows[0].shape[1]
    hidden_units = weights[0].shape[1]
    side = carried[0].shape[1] - width
    total = sum(r.shape[0] for r in rows)
    tables = [
        pl.BlockSpec((c.shape[0], side), lambda i, at=width // side: (0, at)) for c in carried
    ]
    whole = [pl.BlockSpec(r.shape, lambda i: (0, 0)) for r in rows]
    return pl.pallas_call(
        lambda *refs: forward_kernel(experts, len(rows), *refs),
        grid=(1,),
        out_shape=[jax.ShapeDtypeStruct((total // 4, width), jnp.bfloat16)] * 4,
        in_specs=[SMEM] + whole + tables + [pl.BlockSpec(w.shape, lambda i: (0, 0)) for w in weights],
        out_specs=[pl.BlockSpec((total // 4, width), lambda i: (0, 0))] * 4,
        compiler_params=pltpu.CompilerParams(vmem_limit_bytes=28 << 20),
        cost_estimate=pl.CostEstimate(
            flops=6 * total * width * hidden_units, bytes_accessed=10 << 20, transcendentals=0
        ),
        name="expert_forward",
    )(ids, *rows, *carried, *weights)


def expert_backward(ids, carried, stored, weights, experts, width):
    hidden_units = weights[0].shape[1]
    total = sum(r.shape[0] for r in carried)
    blocks = len(carried)
    return pl.pallas_call(
        lambda *refs: backward_kernel(experts, blocks, *refs),
        out_shape=[jax.ShapeDtypeStruct((total // 4, width), jnp.bfloat16)] * 4,
        in_specs=[SMEM] + [VMEM] * (blocks + 4),
        out_specs=[VMEM] * 4,
        compiler_params=pltpu.CompilerParams(vmem_limit_bytes=28 << 20),
        cost_estimate=pl.CostEstimate(
            flops=6 * total * width * hidden_units, bytes_accessed=12 << 20, transcendentals=0
        ),
        name="expert_backward",
    )(ids, *carried, stored, *weights)


def norm_kernel(kept, received, gain, out):
    values = kept[...].astype(jnp.float32) + received[...].astype(jnp.float32)
    out[...] = (values * inverse_rms(values) * gain[...]).astype(jnp.bfloat16)


def normed_rows(kept, received, gain):
    return pl.pallas_call(
        norm_kernel,
        out_shape=jax.ShapeDtypeStruct(kept.shape, jnp.bfloat16),
        in_specs=[VMEM] * 3,
        out_specs=VMEM,
        compiler_params=pltpu.CompilerParams(vmem_limit_bytes=4 << 20),
        cost_estimate=pl.CostEstimate(flops=NORM_FLOPS, bytes_accessed=6 * kept.size, transcendentals=0),
        name="normed_rows",
    )(kept, received, gain)


def gradient_kernel(grad_normed, saved, grad_out, gain, out):
    saved_now = saved[...].astype(jnp.float32)
    scale = inverse_rms(saved_now)
    weighted = grad_normed[...] * gain[...]
    projection = jnp.mean(weighted * saved_now, axis=-1, keepdims=True)
    grad = grad_out[...].astype(jnp.float32) + scale * weighted
    out[...] = (grad - saved_now * scale * scale * scale * projection).astype(jnp.bfloat16)


def gradient_rows(grad_normed, saved, grad_out, gain):
    return pl.pallas_call(
        gradient_kernel,
        out_shape=jax.ShapeDtypeStruct(saved.shape, jnp.bfloat16),
        in_specs=[VMEM] * 4,
        out_specs=VMEM,
        compiler_params=pltpu.CompilerParams(vmem_limit_bytes=8 << 20),
        cost_estimate=pl.CostEstimate(
            flops=16 * saved.size, bytes_accessed=10 * saved.size, transcendentals=0
        ),
        name="gradient_rows",
    )(grad_normed, saved, grad_out, gain)


def dense_weights(routes, probs, experts):
    ids = jnp.arange(experts, dtype=jnp.int32)
    hit = routes[:, :, None] == ids[None, None, :]
    return jnp.sum(jnp.where(hit, probs[:, :, None], 0.0), axis=1)


def in_two(values):
    high = values.astype(jnp.bfloat16)
    low = (values - high.astype(jnp.float32)).astype(jnp.bfloat16)
    return [high, low]


def on_device(
    reference_act,
    codes,
    scale_index,
    scale_table,
    norm_gain,
    routes_fwd,
    probs_fwd,
    gate_weight,
    up_weight,
    down_weight,
    saved_input,
    routes_bwd,
    probs_bwd,
    saved_preact,
    cotangent,
):
    f32, bf16 = jnp.float32, jnp.bfloat16
    experts = lax.axis_size("expert")
    grid = Grid(experts)
    model_width = reference_act.shape[2]
    levels = scale_table.shape[0]
    weights = (gate_weight[0, 0], up_weight[0, 0], down_weight[0, 0])
    stored = saved_preact[0, 0].reshape(experts, -1, saved_preact.shape[3])

    numbers = [grid.numbers(group) for group in grid.groups]
    stored = prepare(jnp.concatenate(numbers), stored)
    grad_out = shifted(cotangent[0], "section", -1)
    picker = (scale_index[0][:, None] == jnp.arange(levels, dtype=jnp.int32)[None, :]).astype(f32)
    row_scale = jnp.sum(picker * scale_table[None, :], axis=1)
    delta_rows = (codes[0].astype(f32) * row_scale[:, None]).astype(bf16)
    received = from_behind(delta_rows, "section", 1)

    table = in_two(dense_weights(routes_fwd[0], probs_fwd[0], experts))
    table += in_two(dense_weights(routes_bwd[0], probs_bwd[0], experts))
    table = jnp.concatenate(table, axis=1)
    table = jnp.pad(table, ((0, 0), (0, -table.shape[1] % 128)))
    carried = grid.gather(jnp.concatenate([grad_out, table], axis=1))

    inputs_now = reference_act[0].astype(f32) + received.astype(f32)
    normed = normed_rows(reference_act[0], received, norm_gain)
    rows = grid.gather(normed)

    slot_grads = []
    for ids, piece in zip(numbers, carried):
        slot_grads.append(
            expert_backward(ids, piece, stored, weights, experts, model_width)
        )
    grad_normed = grid.scatter_sum(slot_grads)
    produced = []
    for ids, piece, side in zip(numbers, rows, carried):
        produced.append(expert_forward(ids, piece, side, weights, experts))
    mixed = inputs_now + grid.scatter_sum(produced)

    grad_now = gradient_rows(grad_normed, saved_input[0], grad_out, norm_gain)
    return (mixed.astype(bf16)[None], grad_now[None])


def solution(mesh):
    step = jax.shard_map(
        on_device,
        mesh=mesh,
        in_specs=(
            P("section", "expert", None),
            P("section", "expert", None),
            P("section", "expert"),
            P(),
            P("section", None),
            P("section", "expert", None),
            P("section", "expert", None),
            P("section", "expert", None, None),
            P("section", "expert", None, None),
            P("section", "expert", None, None),
            P("section", "expert", None),
            P("section", "expert", None),
            P("section", "expert", None),
            P("section", "expert", None, None),
            P("section", "expert", None),
        ),
        out_specs=(P("section", "expert", None), P("section", "expert", None)),
        check_vma=False,
    )
    if Grid(mesh.shape["expert"]).outer > 4:
        return step
    return step
```

```python
import jax
import jax.numpy as jnp
import numpy as np
from jax import lax
from jax.experimental import pallas as pl
from jax.experimental.pallas import tpu as pltpu
from jax.sharding import PartitionSpec as P

EPSILON = 1e-06
NORM_FLOPS = 4_000_000_000
PREPARE_FLOPS = 8_000_000_000


def from_behind(block, axis, distance):
    devices = range(lax.axis_size(axis))
    route = [(i - distance, i) for i in devices if i - distance in devices]
    return lax.ppermute(block, axis, route)


def shifted(x, axis, by):
    size = lax.axis_size(axis)
    return lax.ppermute(x, axis, [(i, (i + by) % size) for i in range(size)])


def inverse_rms(values):
    return lax.rsqrt(jnp.mean(values * values, axis=-1, keepdims=True) + EPSILON)


JOINED = (("b", 0), ("b", 1))


class Grid:
    def __init__(self, size):
        assert size >= 8 and size & (size - 1) == 0
        self.size = size
        self.outer = size // 4
        self.groups = [(k, k + 1) for k in range(0, self.outer, 2)]

    def swap(self, x, bits):
        return lax.ppermute(x, "expert", [(i, i ^ bits) for i in range(self.size)])

    def numbers(self, group):
        flips = [0] + [4 * k + f for f in (0, 2, 1, 3) for k in group]
        return lax.axis_index("expert") ^ np.array(flips, np.int32)

    def gather(self, x):
        near = {0: x}
        for k in range(1, self.outer):
            low = k & -k
            near[k] = self.swap(near[k - low], 4 * low)
        pieces = []
        for group in self.groups:
            own = [near[k] for k in group]
            other, own_beside, other_beside = [], [], []
            for k in group:
                other.append(self.swap(near[k], 2))
                own_beside.append(self.swap(near[k], 1))
                other_beside.append(self.swap(other[-1], 1))
            pieces.append(own + other + own_beside + other_beside)
        return pieces

    def scatter_sum(self, partials, name):
        f32, bf16 = jnp.float32, jnp.bfloat16
        total = {}
        for g, (group, piece) in enumerate(zip(self.groups, partials)):
            own, other, own_beside, other_beside = piece
            other_beside = self.swap(other_beside, 1)
            own_beside = self.swap(own_beside, 1)
            sent = (other.astype(f32) + other_beside.astype(f32)).astype(bf16)
            block = own.shape[0] // len(group)
            near = own.astype(f32) + own_beside.astype(f32)
            if (name, g) in JOINED:
                joined = self.swap(sent[block:], 4)
                sent = (sent[:block].astype(f32) + joined.astype(f32)).astype(bf16)
            crossed = self.swap(sent, 2)
            for i, k in enumerate(group):
                part = slice(i * block, (i + 1) * block)
                total[k] = near[part]
                if part.stop <= crossed.shape[0]:
                    total[k] = total[k] + crossed[part].astype(f32)
        for k in sorted(total, key=lambda k: (-bin(k).count("1"), -k)):
            low = k & -k
            if k:
                part = total[k].astype(bf16)
                part = self.swap(part, 4 * low)
                total[k - low] = total[k - low] + part.astype(f32)
        return total[0]


NT = (((1,), (1,)), ((), ()))
VMEM = pl.BlockSpec(memory_space=pltpu.VMEM)
SMEM = pl.BlockSpec(memory_space=pltpu.SMEM)
ANY = pl.BlockSpec(memory_space=pl.ANY)


def own_weight(table, me, first, experts):
    lane = lax.broadcasted_iota(jnp.int32, table.shape, 1)
    high = first * experts + me
    here = (lane == high) | (lane == high + experts)
    return jnp.sum(jnp.where(here, table, 0.0), axis=1, keepdims=True)


def put_rows(out, outs):
    start = 0
    for ref in outs:
        ref[...] = out[start : start + ref.shape[0]]
        start += ref.shape[0]


def forward_kernel(experts, pieces, ids, *refs):
    f32, bf16 = jnp.float32, jnp.bfloat16
    blocks, tables, refs = refs[:pieces], refs[pieces : 2 * pieces], refs[2 * pieces :]
    wg, wu, wd, oa, ob, oc, od = refs
    table = jnp.concatenate([t[...] for t in tables], axis=0).astype(f32)
    weight = own_weight(table, ids[0], 0, experts)
    rows = jnp.concatenate([r[...] for r in blocks], axis=0)
    gate = jnp.dot(rows, wg[...], preferred_element_type=f32)
    up = jnp.dot(rows, wu[...], preferred_element_type=f32)
    hidden = (gate * jax.nn.sigmoid(gate) * up).astype(bf16)
    out = jnp.dot(hidden, wd[...], preferred_element_type=f32)
    put_rows((out * weight).astype(bf16), (oa, ob, oc, od))


def prepare_kernel(ids, stored, slopes):
    hidden_units = stored.shape[2] // 2

    def block(i, carry):
        kept = stored[i].astype(jnp.float32)
        gate, up = kept[:, :hidden_units], kept[:, hidden_units:]
        sigma = jax.nn.sigmoid(gate)
        slope = up * sigma * (1.0 + gate * (1.0 - sigma))
        slopes[i] = jnp.concatenate([slope, gate * sigma], axis=1).astype(jnp.bfloat16)
        return carry

    lax.fori_loop(0, stored.shape[0], block, 0)


def prepare(ids, stored):
    return pl.pallas_call(
        prepare_kernel,
        out_shape=jax.ShapeDtypeStruct(stored.shape, stored.dtype),
        in_specs=[SMEM, VMEM],
        out_specs=VMEM,
        compiler_params=pltpu.CompilerParams(vmem_limit_bytes=12 << 20),
        cost_estimate=pl.CostEstimate(
            flops=PREPARE_FLOPS, bytes_accessed=4 * stored.size, transcendentals=stored.size
        ),
        name="prepare",
    )(ids, stored)


def backward_kernel(experts, pieces, ids, *refs):
    f32, bf16 = jnp.float32, jnp.bfloat16
    carried, refs = refs[:pieces], refs[pieces:]
    stored, wg, wu, wd, oa, ob, oc, od = refs
    capacity = stored.shape[1]
    tokens = carried[0].shape[0]
    hidden_units = wg.shape[1]
    width = oa.shape[1]
    table = jnp.concatenate([r[:, width:] for r in carried], axis=0).astype(f32)
    weight = own_weight(table, ids[0], 2, experts)
    rows = jnp.concatenate([r[:, :width] for r in carried], axis=0)

    below = lax.broadcasted_iota(jnp.int32, (tokens, tokens), 0)
    below = (below > lax.broadcasted_iota(jnp.int32, (tokens, tokens), 1)).astype(bf16)
    column = lax.broadcasted_iota(jnp.int32, (tokens, capacity), 1).astype(f32)
    grad_hidden = lax.dot_general(rows, wd[...], NT, preferred_element_type=f32)
    grad_gates, grad_ups = [], []
    for i in range(pieces):
        part = slice(i * tokens, (i + 1) * tokens)
        named = weight[part] > 0
        ones = jnp.broadcast_to(jnp.where(named, 1.0, 0.0), (tokens, 128)).astype(bf16)
        earlier = jnp.dot(below, ones, preferred_element_type=f32)[:, :1]
        slot = jnp.where(named, earlier, -1.0)
        pick = (column == slot).astype(f32).astype(bf16)
        placed = jnp.dot(pick, stored[ids[1 + i]], preferred_element_type=f32)
        hidden = grad_hidden[part]
        grad_gates.append((hidden * placed[:, :hidden_units]).astype(bf16))
        grad_ups.append((hidden * placed[:, hidden_units:]).astype(bf16))
    grad_gate = jnp.concatenate(grad_gates, axis=0)
    grad_up = jnp.concatenate(grad_ups, axis=0)
    out = lax.dot_general(grad_gate, wg[...], NT, preferred_element_type=f32)
    out = out + lax.dot_general(grad_up, wu[...], NT, preferred_element_type=f32)
    put_rows((out * weight).astype(bf16), (oa, ob, oc, od))


def expert_forward(ids, rows, carried, weights, experts):
    width = rows[0].shape[1]
    hidden_units = weights[0].shape[1]
    side = carried[0].shape[1] - width
    total = sum(r.shape[0] for r in rows)
    tables = [
        pl.BlockSpec((c.shape[0], side), lambda i, at=width // side: (0, at)) for c in carried
    ]
    whole = [pl.BlockSpec(r.shape, lambda i: (0, 0)) for r in rows]
    return pl.pallas_call(
        lambda *refs: forward_kernel(experts, len(rows), *refs),
        grid=(1,),
        out_shape=[jax.ShapeDtypeStruct((total // 4, width), jnp.bfloat16)] * 4,
        in_specs=[SMEM] + whole + tables + [pl.BlockSpec(w.shape, lambda i: (0, 0)) for w in weights],
        out_specs=[pl.BlockSpec((total // 4, width), lambda i: (0, 0))] * 4,
        compiler_params=pltpu.CompilerParams(vmem_limit_bytes=28 << 20),
        cost_estimate=pl.CostEstimate(
            flops=6 * total * width * hidden_units, bytes_accessed=10 << 20, transcendentals=0
        ),
        name="expert_forward",
    )(ids, *rows, *carried, *weights)


def expert_backward(ids, carried, stored, weights, experts, width):
    hidden_units = weights[0].shape[1]
    total = sum(r.shape[0] for r in carried)
    blocks = len(carried)
    return pl.pallas_call(
        lambda *refs: backward_kernel(experts, blocks, *refs),
        out_shape=[jax.ShapeDtypeStruct((total // 4, width), jnp.bfloat16)] * 4,
        in_specs=[SMEM] + [VMEM] * (blocks + 4),
        out_specs=[VMEM] * 4,
        compiler_params=pltpu.CompilerParams(vmem_limit_bytes=28 << 20),
        cost_estimate=pl.CostEstimate(
            flops=6 * total * width * hidden_units, bytes_accessed=12 << 20, transcendentals=0
        ),
        name="expert_backward",
    )(ids, *carried, stored, *weights)


def norm_kernel(kept, received, gain, out):
    values = kept[...].astype(jnp.float32) + received[...].astype(jnp.float32)
    out[...] = (values * inverse_rms(values) * gain[...]).astype(jnp.bfloat16)


def normed_rows(kept, received, gain):
    return pl.pallas_call(
        norm_kernel,
        out_shape=jax.ShapeDtypeStruct(kept.shape, jnp.bfloat16),
        in_specs=[VMEM] * 3,
        out_specs=VMEM,
        compiler_params=pltpu.CompilerParams(vmem_limit_bytes=4 << 20),
        cost_estimate=pl.CostEstimate(flops=NORM_FLOPS, bytes_accessed=6 * kept.size, transcendentals=0),
        name="normed_rows",
    )(kept, received, gain)


def gradient_kernel(grad_normed, saved, grad_out, gain, out):
    saved_now = saved[...].astype(jnp.float32)
    scale = inverse_rms(saved_now)
    weighted = grad_normed[...] * gain[...]
    projection = jnp.mean(weighted * saved_now, axis=-1, keepdims=True)
    grad = grad_out[...].astype(jnp.float32) + scale * weighted
    out[...] = (grad - saved_now * scale * scale * scale * projection).astype(jnp.bfloat16)


def gradient_rows(grad_normed, saved, grad_out, gain):
    return pl.pallas_call(
        gradient_kernel,
        out_shape=jax.ShapeDtypeStruct(saved.shape, jnp.bfloat16),
        in_specs=[VMEM] * 4,
        out_specs=VMEM,
        compiler_params=pltpu.CompilerParams(vmem_limit_bytes=8 << 20),
        cost_estimate=pl.CostEstimate(
            flops=16 * saved.size, bytes_accessed=10 * saved.size, transcendentals=0
        ),
        name="gradient_rows",
    )(grad_normed, saved, grad_out, gain)


def dense_weights(routes, probs, experts):
    ids = jnp.arange(experts, dtype=jnp.int32)
    hit = routes[:, :, None] == ids[None, None, :]
    return jnp.sum(jnp.where(hit, probs[:, :, None], 0.0), axis=1)


def in_two(values):
    high = values.astype(jnp.bfloat16)
    low = (values - high.astype(jnp.float32)).astype(jnp.bfloat16)
    return [high, low]


def on_device(
    reference_act,
    codes,
    scale_index,
    scale_table,
    norm_gain,
    routes_fwd,
    probs_fwd,
    gate_weight,
    up_weight,
    down_weight,
    saved_input,
    routes_bwd,
    probs_bwd,
    saved_preact,
    cotangent,
):
    f32, bf16 = jnp.float32, jnp.bfloat16
    experts = lax.axis_size("expert")
    grid = Grid(experts)
    model_width = reference_act.shape[2]
    levels = scale_table.shape[0]
    weights = (gate_weight[0, 0], up_weight[0, 0], down_weight[0, 0])
    stored = saved_preact[0, 0].reshape(experts, -1, saved_preact.shape[3])

    numbers = [grid.numbers(group) for group in grid.groups]
    stored = prepare(jnp.concatenate(numbers), stored)
    grad_out = shifted(cotangent[0], "section", -1)
    picker = (scale_index[0][:, None] == jnp.arange(levels, dtype=jnp.int32)[None, :]).astype(f32)
    row_scale = jnp.sum(picker * scale_table[None, :], axis=1)
    delta_rows = (codes[0].astype(f32) * row_scale[:, None]).astype(bf16)
    received = from_behind(delta_rows, "section", 1)

    table = in_two(dense_weights(routes_fwd[0], probs_fwd[0], experts))
    table += in_two(dense_weights(routes_bwd[0], probs_bwd[0], experts))
    table = jnp.concatenate(table, axis=1)
    table = jnp.pad(table, ((0, 0), (0, -table.shape[1] % 128)))
    carried = grid.gather(jnp.concatenate([grad_out, table], axis=1))

    inputs_now = reference_act[0].astype(f32) + received.astype(f32)
    normed = normed_rows(reference_act[0], received, norm_gain)
    rows = grid.gather(normed)

    slot_grads = []
    for ids, piece in zip(numbers, carried):
        slot_grads.append(
            expert_backward(ids, piece, stored, weights, experts, model_width)
        )
    grad_normed = grid.scatter_sum(slot_grads, "b")
    produced = []
    for ids, piece, side in zip(numbers, rows, carried):
        produced.append(expert_forward(ids, piece, side, weights, experts))
    mixed = inputs_now + grid.scatter_sum(produced, "f")

    grad_now = gradient_rows(grad_normed, saved_input[0], grad_out, norm_gain)
    return (mixed.astype(bf16)[None], grad_now[None])


def solution(mesh):
    step = jax.shard_map(
        on_device,
        mesh=mesh,
        in_specs=(
            P("section", "expert", None),
            P("section", "expert", None),
            P("section", "expert"),
            P(),
            P("section", None),
            P("section", "expert", None),
            P("section", "expert", None),
            P("section", "expert", None, None),
            P("section", "expert", None, None),
            P("section", "expert", None, None),
            P("section", "expert", None),
            P("section", "expert", None),
            P("section", "expert", None),
            P("section", "expert", None, None),
            P("section", "expert", None),
        ),
        out_specs=(P("section", "expert", None), P("section", "expert", None)),
        check_vma=False,
    )
    if Grid(mesh.shape["expert"]).outer > 4:
        return step
    return step
```

```python
import jax
import jax.numpy as jnp
import numpy as np
from jax import lax
from jax.experimental import pallas as pl
from jax.experimental.pallas import tpu as pltpu
from jax.sharding import PartitionSpec as P

EPSILON = 1e-06
NORM_FLOPS = 4_000_000_000
PREPARE_FLOPS = 8_000_000_000


def from_behind(block, axis, distance):
    devices = range(lax.axis_size(axis))
    route = [(i - distance, i) for i in devices if i - distance in devices]
    return lax.ppermute(block, axis, route)


def shifted(x, axis, by):
    size = lax.axis_size(axis)
    return lax.ppermute(x, axis, [(i, (i + by) % size) for i in range(size)])


def inverse_rms(values):
    return lax.rsqrt(jnp.mean(values * values, axis=-1, keepdims=True) + EPSILON)


JOINED = (("b", 0), ("b", 1))
PARTED = (("f", 0),)


class Grid:
    def __init__(self, size):
        assert size >= 8 and size & (size - 1) == 0
        self.size = size
        self.outer = size // 4
        self.groups = [(k, k + 1) for k in range(0, self.outer, 2)]

    def swap(self, x, bits):
        return lax.ppermute(x, "expert", [(i, i ^ bits) for i in range(self.size)])

    def numbers(self, group):
        flips = [0] + [4 * k + f for f in (0, 2, 1, 3) for k in group]
        return lax.axis_index("expert") ^ np.array(flips, np.int32)

    def gather(self, x):
        near = {0: x}
        for k in range(1, self.outer):
            low = k & -k
            near[k] = self.swap(near[k - low], 4 * low)
        pieces = []
        for group in self.groups:
            own = [near[k] for k in group]
            other, own_beside, other_beside = [], [], []
            for k in group:
                other.append(self.swap(near[k], 2))
                own_beside.append(self.swap(near[k], 1))
                other_beside.append(self.swap(other[-1], 1))
            pieces.append(own + other + own_beside + other_beside)
        return pieces

    def scatter_sum(self, partials, name):
        f32, bf16 = jnp.float32, jnp.bfloat16
        total = {}
        for g, (group, piece) in enumerate(zip(self.groups, partials)):
            own, other, own_beside, other_beside = piece
            other_beside = self.swap(other_beside, 1)
            own_beside = self.swap(own_beside, 1)
            sent = (other.astype(f32) + other_beside.astype(f32)).astype(bf16)
            block = own.shape[0] // len(group)
            near = own.astype(f32) + own_beside.astype(f32)
            if (name, g) in JOINED:
                joined = self.swap(sent[block:], 4)
                sent = (sent[:block].astype(f32) + joined.astype(f32)).astype(bf16)
            if (name, g) in PARTED:
                last = self.swap(sent[block:], 2)
                sent = sent[:block]
            crossed = self.swap(sent, 2)
            if (name, g) in PARTED:
                crossed = jnp.concatenate([crossed, last], axis=0)
            for i, k in enumerate(group):
                part = slice(i * block, (i + 1) * block)
                total[k] = near[part]
                if part.stop <= crossed.shape[0]:
                    total[k] = total[k] + crossed[part].astype(f32)
        for k in sorted(total, key=lambda k: (-bin(k).count("1"), -k)):
            low = k & -k
            if k:
                part = total[k].astype(bf16)
                part = self.swap(part, 4 * low)
                total[k - low] = total[k - low] + part.astype(f32)
        return total[0]


NT = (((1,), (1,)), ((), ()))
VMEM = pl.BlockSpec(memory_space=pltpu.VMEM)
SMEM = pl.BlockSpec(memory_space=pltpu.SMEM)
ANY = pl.BlockSpec(memory_space=pl.ANY)


def own_weight(table, me, first, experts):
    lane = lax.broadcasted_iota(jnp.int32, table.shape, 1)
    high = first * experts + me
    here = (lane == high) | (lane == high + experts)
    return jnp.sum(jnp.where(here, table, 0.0), axis=1, keepdims=True)


def put_rows(out, outs):
    start = 0
    for ref in outs:
        ref[...] = out[start : start + ref.shape[0]]
        start += ref.shape[0]


def forward_kernel(experts, pieces, ids, *refs):
    f32, bf16 = jnp.float32, jnp.bfloat16
    blocks, tables, refs = refs[:pieces], refs[pieces : 2 * pieces], refs[2 * pieces :]
    wg, wu, wd, oa, ob, oc, od = refs
    table = jnp.concatenate([t[...] for t in tables], axis=0).astype(f32)
    weight = own_weight(table, ids[0], 0, experts)
    rows = jnp.concatenate([r[...] for r in blocks], axis=0)
    gate = jnp.dot(rows, wg[...], preferred_element_type=f32)
    up = jnp.dot(rows, wu[...], preferred_element_type=f32)
    hidden = (gate * jax.nn.sigmoid(gate) * up).astype(bf16)
    out = jnp.dot(hidden, wd[...], preferred_element_type=f32)
    put_rows((out * weight).astype(bf16), (oa, ob, oc, od))


def prepare_kernel(ids, stored, slopes):
    hidden_units = stored.shape[2] // 2

    def block(i, carry):
        kept = stored[i].astype(jnp.float32)
        gate, up = kept[:, :hidden_units], kept[:, hidden_units:]
        sigma = jax.nn.sigmoid(gate)
        slope = up * sigma * (1.0 + gate * (1.0 - sigma))
        slopes[i] = jnp.concatenate([slope, gate * sigma], axis=1).astype(jnp.bfloat16)
        return carry

    lax.fori_loop(0, stored.shape[0], block, 0)


def prepare(ids, stored):
    return pl.pallas_call(
        prepare_kernel,
        out_shape=jax.ShapeDtypeStruct(stored.shape, stored.dtype),
        in_specs=[SMEM, VMEM],
        out_specs=VMEM,
        compiler_params=pltpu.CompilerParams(vmem_limit_bytes=12 << 20),
        cost_estimate=pl.CostEstimate(
            flops=PREPARE_FLOPS, bytes_accessed=4 * stored.size, transcendentals=stored.size
        ),
        name="prepare",
    )(ids, stored)


def backward_kernel(experts, pieces, ids, *refs):
    f32, bf16 = jnp.float32, jnp.bfloat16
    carried, refs = refs[:pieces], refs[pieces:]
    stored, wg, wu, wd, oa, ob, oc, od = refs
    capacity = stored.shape[1]
    tokens = carried[0].shape[0]
    hidden_units = wg.shape[1]
    width = oa.shape[1]
    table = jnp.concatenate([r[:, width:] for r in carried], axis=0).astype(f32)
    weight = own_weight(table, ids[0], 2, experts)
    rows = jnp.concatenate([r[:, :width] for r in carried], axis=0)

    below = lax.broadcasted_iota(jnp.int32, (tokens, tokens), 0)
    below = (below > lax.broadcasted_iota(jnp.int32, (tokens, tokens), 1)).astype(bf16)
    column = lax.broadcasted_iota(jnp.int32, (tokens, capacity), 1).astype(f32)
    grad_hidden = lax.dot_general(rows, wd[...], NT, preferred_element_type=f32)
    grad_gates, grad_ups = [], []
    for i in range(pieces):
        part = slice(i * tokens, (i + 1) * tokens)
        named = weight[part] > 0
        ones = jnp.broadcast_to(jnp.where(named, 1.0, 0.0), (tokens, 128)).astype(bf16)
        earlier = jnp.dot(below, ones, preferred_element_type=f32)[:, :1]
        slot = jnp.where(named, earlier, -1.0)
        pick = (column == slot).astype(f32).astype(bf16)
        placed = jnp.dot(pick, stored[ids[1 + i]], preferred_element_type=f32)
        hidden = grad_hidden[part]
        grad_gates.append((hidden * placed[:, :hidden_units]).astype(bf16))
        grad_ups.append((hidden * placed[:, hidden_units:]).astype(bf16))
    grad_gate = jnp.concatenate(grad_gates, axis=0)
    grad_up = jnp.concatenate(grad_ups, axis=0)
    out = lax.dot_general(grad_gate, wg[...], NT, preferred_element_type=f32)
    out = out + lax.dot_general(grad_up, wu[...], NT, preferred_element_type=f32)
    put_rows((out * weight).astype(bf16), (oa, ob, oc, od))


def expert_forward(ids, rows, carried, weights, experts):
    width = rows[0].shape[1]
    hidden_units = weights[0].shape[1]
    side = carried[0].shape[1] - width
    total = sum(r.shape[0] for r in rows)
    tables = [
        pl.BlockSpec((c.shape[0], side), lambda i, at=width // side: (0, at)) for c in carried
    ]
    whole = [pl.BlockSpec(r.shape, lambda i: (0, 0)) for r in rows]
    return pl.pallas_call(
        lambda *refs: forward_kernel(experts, len(rows), *refs),
        grid=(1,),
        out_shape=[jax.ShapeDtypeStruct((total // 4, width), jnp.bfloat16)] * 4,
        in_specs=[SMEM] + whole + tables + [pl.BlockSpec(w.shape, lambda i: (0, 0)) for w in weights],
        out_specs=[pl.BlockSpec((total // 4, width), lambda i: (0, 0))] * 4,
        compiler_params=pltpu.CompilerParams(vmem_limit_bytes=28 << 20),
        cost_estimate=pl.CostEstimate(
            flops=6 * total * width * hidden_units, bytes_accessed=10 << 20, transcendentals=0
        ),
        name="expert_forward",
    )(ids, *rows, *carried, *weights)


def expert_backward(ids, carried, stored, weights, experts, width):
    hidden_units = weights[0].shape[1]
    total = sum(r.shape[0] for r in carried)
    blocks = len(carried)
    return pl.pallas_call(
        lambda *refs: backward_kernel(experts, blocks, *refs),
        out_shape=[jax.ShapeDtypeStruct((total // 4, width), jnp.bfloat16)] * 4,
        in_specs=[SMEM] + [VMEM] * (blocks + 4),
        out_specs=[VMEM] * 4,
        compiler_params=pltpu.CompilerParams(vmem_limit_bytes=28 << 20),
        cost_estimate=pl.CostEstimate(
            flops=6 * total * width * hidden_units, bytes_accessed=12 << 20, transcendentals=0
        ),
        name="expert_backward",
    )(ids, *carried, stored, *weights)


def norm_kernel(kept, received, gain, out):
    values = kept[...].astype(jnp.float32) + received[...].astype(jnp.float32)
    out[...] = (values * inverse_rms(values) * gain[...]).astype(jnp.bfloat16)


def normed_rows(kept, received, gain):
    return pl.pallas_call(
        norm_kernel,
        out_shape=jax.ShapeDtypeStruct(kept.shape, jnp.bfloat16),
        in_specs=[VMEM] * 3,
        out_specs=VMEM,
        compiler_params=pltpu.CompilerParams(vmem_limit_bytes=4 << 20),
        cost_estimate=pl.CostEstimate(flops=NORM_FLOPS, bytes_accessed=6 * kept.size, transcendentals=0),
        name="normed_rows",
    )(kept, received, gain)


def gradient_kernel(grad_normed, saved, grad_out, gain, out):
    saved_now = saved[...].astype(jnp.float32)
    scale = inverse_rms(saved_now)
    weighted = grad_normed[...] * gain[...]
    projection = jnp.mean(weighted * saved_now, axis=-1, keepdims=True)
    grad = grad_out[...].astype(jnp.float32) + scale * weighted
    out[...] = (grad - saved_now * scale * scale * scale * projection).astype(jnp.bfloat16)


def gradient_rows(grad_normed, saved, grad_out, gain):
    return pl.pallas_call(
        gradient_kernel,
        out_shape=jax.ShapeDtypeStruct(saved.shape, jnp.bfloat16),
        in_specs=[VMEM] * 4,
        out_specs=VMEM,
        compiler_params=pltpu.CompilerParams(vmem_limit_bytes=8 << 20),
        cost_estimate=pl.CostEstimate(
            flops=16 * saved.size, bytes_accessed=10 * saved.size, transcendentals=0
        ),
        name="gradient_rows",
    )(grad_normed, saved, grad_out, gain)


def dense_weights(routes, probs, experts):
    ids = jnp.arange(experts, dtype=jnp.int32)
    hit = routes[:, :, None] == ids[None, None, :]
    return jnp.sum(jnp.where(hit, probs[:, :, None], 0.0), axis=1)


def in_two(values):
    high = values.astype(jnp.bfloat16)
    low = (values - high.astype(jnp.float32)).astype(jnp.bfloat16)
    return [high, low]


def on_device(
    reference_act,
    codes,
    scale_index,
    scale_table,
    norm_gain,
    routes_fwd,
    probs_fwd,
    gate_weight,
    up_weight,
    down_weight,
    saved_input,
    routes_bwd,
    probs_bwd,
    saved_preact,
    cotangent,
):
    f32, bf16 = jnp.float32, jnp.bfloat16
    experts = lax.axis_size("expert")
    grid = Grid(experts)
    model_width = reference_act.shape[2]
    levels = scale_table.shape[0]
    weights = (gate_weight[0, 0], up_weight[0, 0], down_weight[0, 0])
    stored = saved_preact[0, 0].reshape(experts, -1, saved_preact.shape[3])

    numbers = [grid.numbers(group) for group in grid.groups]
    stored = prepare(jnp.concatenate(numbers), stored)
    grad_out = shifted(cotangent[0], "section", -1)
    picker = (scale_index[0][:, None] == jnp.arange(levels, dtype=jnp.int32)[None, :]).astype(f32)
    row_scale = jnp.sum(picker * scale_table[None, :], axis=1)
    delta_rows = (codes[0].astype(f32) * row_scale[:, None]).astype(bf16)
    received = from_behind(delta_rows, "section", 1)

    table = in_two(dense_weights(routes_fwd[0], probs_fwd[0], experts))
    table += in_two(dense_weights(routes_bwd[0], probs_bwd[0], experts))
    table = jnp.concatenate(table, axis=1)
    table = jnp.pad(table, ((0, 0), (0, -table.shape[1] % 128)))
    carried = grid.gather(jnp.concatenate([grad_out, table], axis=1))

    inputs_now = reference_act[0].astype(f32) + received.astype(f32)
    normed = normed_rows(reference_act[0], received, norm_gain)
    rows = grid.gather(normed)

    slot_grads = []
    for ids, piece in zip(numbers, carried):
        slot_grads.append(
            expert_backward(ids, piece, stored, weights, experts, model_width)
        )
    grad_normed = grid.scatter_sum(slot_grads, "b")
    produced = []
    for ids, piece, side in zip(numbers, rows, carried):
        produced.append(expert_forward(ids, piece, side, weights, experts))
    mixed = inputs_now + grid.scatter_sum(produced, "f")

    grad_now = gradient_rows(grad_normed, saved_input[0], grad_out, norm_gain)
    return (mixed.astype(bf16)[None], grad_now[None])


def solution(mesh):
    step = jax.shard_map(
        on_device,
        mesh=mesh,
        in_specs=(
            P("section", "expert", None),
            P("section", "expert", None),
            P("section", "expert"),
            P(),
            P("section", None),
            P("section", "expert", None),
            P("section", "expert", None),
            P("section", "expert", None, None),
            P("section", "expert", None, None),
            P("section", "expert", None, None),
            P("section", "expert", None),
            P("section", "expert", None),
            P("section", "expert", None),
            P("section", "expert", None, None),
            P("section", "expert", None),
        ),
        out_specs=(P("section", "expert", None), P("section", "expert", None)),
        check_vma=False,
    )
    if Grid(mesh.shape["expert"]).outer > 4:
        return step
    return step
```
